256 devices in a mesh: dp: 8 (over y, core), seq: 32 (over z, x).
Axes of the slice: x: 4, y: 4, z: 8, core: 2. Of those that a mesh axis runs over, the one named last changes fastest.
Arguments:
- queries: bfloat16 [64, 2048, 2048], P('dp', 'seq'), may hold values from -6 to 6
- enc_keys: bfloat16 [64, 2048, 2048], P('dp', 'seq'), may hold values from -6 to 6
- enc_values: bfloat16 [64, 2048, 2048], P('dp', 'seq'), may hold values from -6 to 6
- dec_ids: int32 [64, 2048], P('dp', 'seq'), may hold values from 0 to 15, never falling along the last dimension, each value on 1 to 512 neighbouring positions
- enc_ids: int32 [64, 2048], P('dp', 'seq'), may hold values from 0 to 15, never falling along the last dimension, each value on 1 to 512 neighbouring positions
Outputs:
- context: bfloat16 [64, 2048, 2048], P('dp', 'seq')
The draws below stay inside these ranges and needn't reach their ends.
Inputs may be any that keep to these rules, and one draw needn't show every extreme that they name: `dec_ids`: along each row the numbers never fall; every number from 0 to 15 occurs in every row; a document holds 1 to 512 positions of a row, and some document holds exactly 512. `enc_ids`: along each row the numbers never fall; every number from 0 to 15 occurs in every row; a document holds 1 to 512 positions of a row, and some document holds exactly 512.
All inputs are finite; a program needn't handle non-finite values.
Results may differ from the reference program's by a relative error of at most 0.0047.
Values may be sent and summed in bfloat16 or wider, within the bound.
A program may use at most 128 MiB of HBM per device.

```python
import math
import jax
import jax.numpy as jnp
import numpy as np
from jax import lax

HEAD_DIM = 64
LEN = 2048
NDOC = 16
MOST = 512
HEADS = 32
INNER = 2048
BATCH = 64


def draw_queries(key, part):
    base = jax.random.truncated_normal(jax.random.fold_in(key, 1), -6.0, 6.0, (BATCH, LEN, HEADS * HEAD_DIM), jnp.float32)
    result = 0.25 * base
    return result.astype(jnp.bfloat16)


def draw_enc_keys(key, part):
    base = jax.random.truncated_normal(jax.random.fold_in(key, 3), -6.0, 6.0, (BATCH, LEN, HEADS * HEAD_DIM), jnp.float32)
    result = base
    return result.astype(jnp.bfloat16)


def levels(rng, dims, cuts, least, top_value):
    level, own = 1.0, jax.random.fold_in(rng, 6)
    for dim, parts in cuts:
        heights = jnp.exp(jax.random.uniform(jax.random.fold_in(own, dim), (parts,), jnp.float32, least / len(cuts), top_value / len(cuts)))
        level = level * jnp.repeat(heights, dims[dim] // parts).reshape([-1 if axis == dim else 1 for axis in range(len(dims))])
    return level


def split_up(amount, total, most, lean):
    weights = [(1 << 20) // math.isqrt(grade ** lean) + 1 for grade in range(2, amount + 1)]
    surplus, given = total - most - (amount - 1), [1] * (amount - 1)
    while surplus > 0:
        free = [i for i in range(amount - 1) if given[i] < most]
        pool, left = sum([weights[i] for i in free]), surplus
        for i in free:
            addition = min(most - given[i], max(1, left * weights[i] // pool), surplus)
            given[i] = given[i] + addition
            surplus = surplus - addition
    return np.array([most] + given)


def uneven_parts(stream_key, number_of, total, most, slope):
    if number_of == 2:
        one = jax.random.randint(stream_key, (), max(1, total - most), min(most, total - 1) + 1)
        return jnp.stack([one, total - one])
    sizes = jnp.asarray(split_up(number_of, total, most, slope), jnp.int32)
    pairs = (number_of - 1) // 2
    giver, sink = sizes[1:1 + 2 * pairs:2], sizes[2:2 + 2 * pairs:2]
    slack = jnp.minimum(giver - 1, most - sink)
    moved = jax.random.randint(jax.random.fold_in(stream_key, 1), (pairs,), 0, 1 << 20) % (slack + 1)
    sizes = sizes.at[1:1 + 2 * pairs:2].set(giver - moved).at[2:2 + 2 * pairs:2].set(sink + moved)
    return sizes[jax.random.permutation(jax.random.fold_in(stream_key, 2), number_of)]


def scatter_about(key, extent, scale, reach, shards=(), kind=jnp.bfloat16):
    factor_of = levels(key, extent, shards, -0.22, 0.18) if shards else 1.0
    values = jax.random.normal(key, extent, jnp.float32) * scale * factor_of
    return jnp.minimum(jnp.maximum(values, -reach), reach).astype(kind)


def setup_inputs(seed: int = 0) -> dict:
    splits = jax.random.split(jax.random.key(seed), 6)
    return {
        "queries": draw_queries(jax.random.fold_in(splits[5], 71), 0),
        "enc_keys": draw_enc_keys(jax.random.fold_in(splits[5], 71), 0),
        "enc_values": scatter_about(splits[2], (BATCH, LEN, INNER), 1.0, 6.0, ((0, 8), (1, 32))),
        "dec_ids": jax.vmap(lambda own: jnp.searchsorted(jnp.cumsum(uneven_parts(own, NDOC, LEN, MOST, 2)), jnp.arange(LEN), side="right"))(jax.random.split(splits[3], BATCH)).reshape((BATCH, LEN)).astype(jnp.int32),
        "enc_ids": jax.vmap(lambda own: jnp.searchsorted(jnp.cumsum(uneven_parts(own, NDOC, LEN, MOST, 2)), jnp.arange(LEN), side="right"))(jax.random.split(splits[4], BATCH)).reshape((BATCH, LEN)).astype(jnp.int32),
    }


masked_score = -1.0e30


def attend_row(query_row, key_row, value_row, dec_row, enc_row):
    query_heads = query_row.astype(jnp.float32).reshape(LEN, HEADS, HEAD_DIM)
    key_heads = key_row.astype(jnp.float32).reshape(LEN, HEADS, HEAD_DIM)
    value_heads = value_row.astype(jnp.float32).reshape(LEN, HEADS, HEAD_DIM)
    query_span = min(512, LEN)
    pieces = []
    for offset in range(0, LEN, query_span):
        scores = jnp.einsum("qhd,khd->hqk", query_heads[offset:offset + query_span], key_heads,
                            precision=lax.Precision.HIGHEST)
        allowed = (dec_row[offset:offset + query_span][:, None] == enc_row[None, :])[None]
        scores = jnp.where(allowed, scores, masked_score)
        row_peak = jnp.max(scores, axis=2, keepdims=True)
        expos = jnp.where(allowed, jnp.exp(scores - row_peak), 0.0)
        row_total = jnp.sum(expos, axis=2, keepdims=True)
        weights = (expos / row_total).astype(jnp.bfloat16)
        weights = lax.optimization_barrier(weights).astype(jnp.float32)
        summed = jnp.einsum("hqk,khd->qhd", weights, value_heads, precision=lax.Precision.HIGHEST)
        pieces.append(summed.reshape(query_span, HEADS * HEAD_DIM).astype(jnp.bfloat16))
    return jnp.concatenate(pieces, axis=0)


def reference(queries, enc_keys, enc_values, dec_ids, enc_ids):
    def one_row(members):
        return attend_row(members[0], members[1], members[2], members[3], members[4])

    return lax.map(one_row, (queries, enc_keys, enc_values, dec_ids, enc_ids))
```

```python
import functools

import jax
import jax.numpy as jnp
from jax import lax
from jax.experimental import pallas as pl
from jax.experimental.pallas import tpu as pltpu
from jax.sharding import PartitionSpec as P

HEAD_DIM = 64
LANES = 128
NDOC = 16
FAR = -float(2**30)
MESH = pl.DeviceIdType.MESH


def doc_counts(ids, base, lane):
    counts = jnp.zeros((ids.shape[0], LANES), jnp.int32)
    slot = lane % HEAD_DIM
    for d in range(NDOC + 1):
        below = jnp.sum(jnp.where(ids < d, 1, 0), axis=1, keepdims=True)
        counts = jnp.where(slot == base + d, below, counts)
    return counts


def kernel(
    size, q_ref, k_ref, v_ref, dec_ref, enc_ref, out_ref,
    q_buf, k_buf, v_buf, o_buf, k_aug, cnt, gath, edges,
    send_sem, recv_sem, cnt_send_sem, cnt_sem, out_send_sem, out_sem,
):
    me = lax.axis_index("seq")
    rows, span = q_buf.shape[0], q_ref.shape[1]
    length = q_buf.shape[1]
    block = min(256, length)
    per_block = block // span
    n_blocks = length // block
    my_pair, my_half = me // 2, lax.rem(me, 2)

    def other(o):
        return lax.rem(me + o, size)

    def lanes_of(t):
        return pl.ds(pl.multiple_of((t // 2) * LANES, LANES), LANES)

    def span_of(t):
        return pl.ds(pl.multiple_of(t * span, span), span)

    barrier = pltpu.get_barrier_semaphore()

    def greet(o, carry):
        pl.semaphore_signal(barrier, inc=1, device_id={"seq": other(o)}, device_id_type=MESH)
        return carry

    lax.fori_loop(1, size, greet, 0)

    arrays = ((k_ref, k_buf), (q_ref, q_buf), (v_ref, v_buf))

    def landing(buf, r, where):
        return buf.at[r, where, pl.ds(0, LANES)]

    for r in range(rows):
        for a, (src, dst) in enumerate(arrays):
            pltpu.make_async_copy(
                src.at[my_half * rows + r, :, lanes_of(me)],
                landing(dst, r, span_of(me)),
                recv_sem.at[r, a],
            ).start()

    lane8 = lax.broadcasted_iota(jnp.int32, (2 * rows, LANES), 1)
    counts = doc_counts(dec_ref[...], 0, lane8) + doc_counts(enc_ref[...], 32, lane8)
    cnt[0] = counts[:rows]
    cnt[1] = counts[rows:]
    gath[me] = jnp.where(my_half == 0, counts[:rows], counts[rows:])
    v_buf[:, :, LANES:] = jnp.ones((rows, length, LANES), jnp.bfloat16)

    pl.semaphore_wait(barrier, size - 1)

    def send_counts(o, carry):
        t = other(o)
        pltpu.make_async_remote_copy(
            src_ref=cnt.at[lax.rem(t, 2)], dst_ref=gath.at[me],
            send_sem=cnt_send_sem, recv_sem=cnt_sem, device_id={"seq": t}, device_id_type=MESH,
        ).start()
        return carry

    lax.fori_loop(1, size, send_counts, 0)

    for r in range(rows):
        for a, (src, dst) in enumerate(arrays):
            def send(o, carry, r=r, a=a, src=src, dst=dst):
                t = other(o)
                pltpu.make_async_remote_copy(
                    src_ref=src.at[lax.rem(t, 2) * rows + r, :, lanes_of(t)],
                    dst_ref=landing(dst, r, span_of(me)),
                    send_sem=send_sem.at[r, a], recv_sem=recv_sem.at[r, a],
                    device_id={"seq": t}, device_id_type=MESH,
                ).start()
                return carry

            lax.fori_loop(1, size, send, 0)

    others = gath.at[pl.ds(0, size - 1)]
    pltpu.make_async_copy(others, others, cnt_sem).wait()
    total = jnp.sum(gath[...], axis=0)
    lane4 = lax.broadcasted_iota(jnp.int32, (rows, LANES), 1)
    real = lane4 % HEAD_DIM < NDOC
    encs = pltpu.roll(total, LANES - 32, 1)
    edges[0] = jnp.where(real, total, 2 * length)
    edges[1] = jnp.where(real, pltpu.roll(total, LANES - 1, 1), 0)
    edges[2] = jnp.where(real, encs, 2 * length)
    edges[3] = jnp.where(real, pltpu.roll(encs, LANES - 1, 1), 0)

    def inside(first, r, start, count):
        pos = lax.broadcasted_iota(jnp.int32, (count, LANES), 0) + start
        low = edges[first, pl.ds(r, 1), :]
        high = edges[first + 1, pl.ds(r, 1), :]
        return (pos >= low) & (pos < high)

    def out_copies(r, blk):
        for i in range(per_block):
            t = blk * per_block + i
            src = o_buf.at[r, span_of(t), :]
            dst = out_ref.at[my_half * rows + r, :, lanes_of(me)]

            @pl.when(t != me)
            def _():
                pltpu.make_async_remote_copy(
                    src_ref=src, dst_ref=dst, send_sem=out_send_sem.at[r], recv_sem=out_sem,
                    device_id={"seq": t}, device_id_type=MESH,
                ).start()

            @pl.when(t == me)
            def _():
                pltpu.make_async_copy(src, dst, out_sem).start()

    left = lax.broadcasted_iota(jnp.int32, (block, LANES), 1) < HEAD_DIM

    def attend_row(r, carry):
        for a, (_, dst) in enumerate(arrays):
            here = landing(dst, r, pl.ds(0, length))
            pltpu.make_async_copy(here, here, recv_sem.at[r, a]).wait()

        def widen(c, inner):
            at = pl.ds(pl.multiple_of(c * block, block), block)
            keys = k_buf[r, at, :]
            apart = jnp.where(inside(2, r, c * block, block), 0.0, FAR).astype(jnp.bfloat16)
            k_aug[0, at, :] = jnp.where(left, keys, apart)
            k_aug[1, at, :] = jnp.where(left, apart, keys)
            return inner

        lax.fori_loop(0, n_blocks, widen, 0)

        def attend_block(blk, inner):
            at = pl.ds(pl.multiple_of(blk * block, block), block)
            mine = q_buf[r, at, :]
            member = jnp.where(inside(0, r, blk * block, block), 1.0, 0.0).astype(jnp.bfloat16)
            values = v_buf[r]
            heads = []
            for h in range(2):
                ask = jnp.where(left, mine, member) if h == 0 else jnp.where(left, member, mine)
                scores = lax.dot_general(
                    ask, k_aug[h], (((1,), (1,)), ((), ())), preferred_element_type=jnp.float32
                )
                peak = jnp.max(scores, axis=1, keepdims=True)
                expos = jnp.exp(scores - peak).astype(jnp.bfloat16)
                summed = jnp.dot(expos, values, preferred_element_type=jnp.float32)
                heads.append(summed[:, :LANES] / summed[:, LANES:])
            o_buf[r, at, :] = jnp.where(left, heads[0], heads[1]).astype(jnp.bfloat16)

            @pl.when(blk > 0)
            def _():
                out_copies(r, blk - 1)

            return inner

        lax.fori_loop(0, n_blocks, attend_block, 0)
        out_copies(r, n_blocks - 1)
        return carry

    lax.fori_loop(0, rows, attend_row, 0)

    pltpu.make_async_copy(others, others, cnt_send_sem).wait()
    for r in range(rows):
        for a, (_, dst) in enumerate(arrays):
            most = landing(dst, r, pl.ds(0, length - span))
            pltpu.make_async_copy(most, most, send_sem.at[r, a]).wait()
        most = o_buf.at[r, pl.ds(0, length - span), :]
        pltpu.make_async_copy(most, most, out_send_sem.at[r]).wait()
    pltpu.make_async_copy(out_ref, out_ref, out_sem).wait()


def local(queries, enc_keys, enc_values, dec_ids, enc_ids):
    size = lax.axis_size("seq")
    batch, span, inner = queries.shape
    rows, length = batch // 2, span * size
    anywhere = pl.BlockSpec(memory_space=pl.ANY)
    vmem = pl.BlockSpec(memory_space=pltpu.VMEM)
    return pl.pallas_call(
        functools.partial(kernel, size),
        out_shape=jax.ShapeDtypeStruct(queries.shape, queries.dtype),
        in_specs=[anywhere, anywhere, anywhere, vmem, vmem],
        out_specs=anywhere,
        scratch_shapes=[
            pltpu.VMEM((rows, length, LANES), jnp.bfloat16),
            pltpu.VMEM((rows, length, LANES), jnp.bfloat16),
            pltpu.VMEM((rows, length, 2 * LANES), jnp.bfloat16),
            pltpu.VMEM((rows, length, LANES), jnp.bfloat16),
            pltpu.VMEM((2, length, LANES), jnp.bfloat16),
            pltpu.VMEM((2, rows, LANES), jnp.int32),
            pltpu.VMEM((size, rows, LANES), jnp.int32),
            pltpu.VMEM((4, rows, LANES), jnp.int32),
            pltpu.SemaphoreType.DMA((rows, 3)),
            pltpu.SemaphoreType.DMA((rows, 3)),
            pltpu.SemaphoreType.DMA,
            pltpu.SemaphoreType.DMA,
            pltpu.SemaphoreType.DMA((rows,)),
            pltpu.SemaphoreType.DMA,
        ],
        compiler_params=pltpu.CompilerParams(
            collective_id=0, has_side_effects=True, vmem_limit_bytes=60 * 1024 * 1024
        ),
    )(queries, enc_keys, enc_values, dec_ids, enc_ids)


def solution(mesh):
    spec, id_spec = P("dp", "seq", None), P("dp", "seq")
    return jax.shard_map(
        local, mesh=mesh, in_specs=(spec, spec, spec, id_spec, id_spec), out_specs=spec, check_vma=False
    )
```

```python
import functools

import jax
import jax.numpy as jnp
from jax import lax
from jax.experimental import pallas as pl
from jax.experimental.pallas import tpu as pltpu
from jax.sharding import PartitionSpec as P

HEAD_DIM = 64
LANES = 128
NDOC = 16
RING_X = 4
FAR = -float(2**30)
MESH = pl.DeviceIdType.MESH


def doc_counts(ids, base, slot):
    counts = jnp.zeros((ids.shape[0], LANES), jnp.int32)
    for d in range(1, NDOC):
        below = jnp.sum(jnp.where(ids < d, 1, 0), axis=1, keepdims=True)
        counts = jnp.where(slot == base + d, below, counts)
    return counts


def kernel(
    size, q_ref, k_ref, v_ref, dec_ref, enc_ref, out_ref,
    q_buf, k_buf, v_buf, o_buf, k_aug, cnt, gath, edges,
    send_sem, recv_sem, cnt_send_sem, cnt_sem, out_send_sem, out_sem, round_sem,
):
    me = lax.axis_index("seq")
    rows, span = q_buf.shape[0], q_ref.shape[1]
    length = q_buf.shape[1]
    block = min(256, length)
    per_block = block // span
    n_blocks = length // block
    my_half = lax.rem(me, 2)
    ring_z, rounds = size // RING_X, round_sem.shape[0]

    def lanes_of(t):
        return pl.ds(pl.multiple_of((t // 2) * LANES, LANES), LANES)

    def span_of(t):
        return pl.ds(pl.multiple_of(t * span, span), span)

    def place(dz, dx):
        return lax.rem(me // RING_X + dz, ring_z) * RING_X + lax.rem(lax.rem(me, RING_X) + dx, RING_X)

    neighbours = (place(1, 0), place(ring_z - 1, 0), place(0, 1), place(0, RING_X - 1))

    def greet(sem):
        for t in neighbours:
            pl.semaphore_signal(sem, inc=1, device_id={"seq": t}, device_id_type=MESH)

    barrier = pltpu.get_barrier_semaphore()
    greet(barrier)

    arrays = ((k_ref, k_buf), (q_ref, q_buf), (v_ref, v_buf))

    def landing(buf, r, where):
        return buf.at[r, where, pl.ds(0, LANES)]

    for r in range(rows):
        for a, (src, dst) in enumerate(arrays):
            pltpu.make_async_copy(
                src.at[my_half * rows + r, :, lanes_of(me)],
                landing(dst, r, span_of(me)),
                recv_sem.at[r, a],
            ).start()

    lane8 = lax.broadcasted_iota(jnp.int32, (2 * rows, LANES), 1)
    row8 = lax.broadcasted_iota(jnp.int32, (2 * rows, LANES), 0)
    counts = doc_counts(dec_ref[...], 0, lane8 % (2 * NDOC)) + doc_counts(enc_ref[...], NDOC, lane8 % (2 * NDOC))
    for half in range(2):
        kept = (row8 // rows == half) & (lane8 // (2 * NDOC) == row8 % rows)
        line = jnp.sum(jnp.where(kept, counts, 0), axis=0, keepdims=True)
        cnt[half] = line

        @pl.when(my_half == half)
        def _():
            gath[me] = line
    def send_counts(t):
        pltpu.make_async_remote_copy(
            src_ref=cnt.at[lax.rem(t, 2)], dst_ref=gath.at[me],
            send_sem=cnt_send_sem, recv_sem=cnt_sem, device_id={"seq": t}, device_id_type=MESH,
        ).start()

    def send(t, r, a):
        src, dst = arrays[a]
        pltpu.make_async_remote_copy(
            src_ref=src.at[lax.rem(t, 2) * rows + r, :, lanes_of(t)],
            dst_ref=landing(dst, r, span_of(me)),
            send_sem=send_sem.at[r, a], recv_sem=recv_sem.at[r, a],
            device_id={"seq": t}, device_id_type=MESH,
        ).start()

    def each_at(nearest, farthest, act):
        def step(o, carry):
            dz, dx = o // RING_X, lax.rem(o, RING_X)
            hops = jnp.minimum(dz, ring_z - dz) + jnp.minimum(dx, RING_X - dx)

            @pl.when((hops >= nearest) & (hops <= farthest))
            def _():
                act(place(dz, dx))

            return carry

        lax.fori_loop(1, size, step, 0)

    def send_row(r, nearest, farthest):
        for a in range(3):
            each_at(nearest, farthest, lambda t: send(t, r, a))

    pl.semaphore_wait(barrier, 4)
    greet(round_sem.at[0])
    for t in neighbours:
        send_counts(t)
    for r in range(rows):
        for a in range(3):
            for t in neighbours:
                send(t, r, a)
    pl.semaphore_wait(round_sem.at[0], 4)
    greet(round_sem.at[1])
    each_at(2, 2, send_counts)
    send_row(0, 2, 2)
    for k in range(1, rounds):
        pl.semaphore_wait(round_sem.at[k], 4)
        if k + 1 < rounds:
            greet(round_sem.at[k + 1])
    each_at(3, size, send_counts)
    send_row(0, 3, size)
    for r in range(1, rows):
        send_row(r, 2, size)
    v_buf[:, :, LANES:] = jnp.ones((rows, length, LANES), jnp.bfloat16)

    others = gath.at[pl.ds(0, size - 1)]
    pltpu.make_async_copy(others, others, cnt_sem).wait()
    total = jnp.broadcast_to(jnp.sum(gath[...], axis=0), (8, LANES))
    slot = lax.broadcasted_iota(jnp.int32, (8, LANES), 1)
    for r in range(rows):
        for which in range(2):
            base = (2 * r + which) * NDOC
            low = pltpu.roll(total, (LANES - base) % LANES, 1)
            low = jnp.where(slot < HEAD_DIM, low, pltpu.roll(low, HEAD_DIM, 1))
            high = jnp.where(slot % HEAD_DIM == NDOC - 1, length, pltpu.roll(low, LANES - 1, 1))
            real = slot % HEAD_DIM < NDOC
            edges[2 * which, pl.ds(r, 1), :] = jnp.where(real, low, 2 * length)[:1]
            edges[2 * which + 1, pl.ds(r, 1), :] = jnp.where(real, high, 0)[:1]

    def inside(first, r, start, count):
        pos = lax.broadcasted_iota(jnp.int32, (count, LANES), 0) + start
        low = edges[first, pl.ds(r, 1), :]
        high = edges[first + 1, pl.ds(r, 1), :]
        return (pos >= low) & (pos < high)

    def out_copies(r, blk):
        for i in range(per_block):
            t = blk * per_block + i
            src = o_buf.at[r, span_of(t), :]
            dst = out_ref.at[my_half * rows + r, :, lanes_of(me)]

            @pl.when(t != me)
            def _():
                pltpu.make_async_remote_copy(
                    src_ref=src, dst_ref=dst, send_sem=out_send_sem.at[r], recv_sem=out_sem,
                    device_id={"seq": t}, device_id_type=MESH,
                ).start()

            @pl.when(t == me)
            def _():
                out_ref[my_half * rows + r, :, lanes_of(me)] = o_buf[r, span_of(me), :]

    left = lax.broadcasted_iota(jnp.int32, (block, LANES), 1) < HEAD_DIM

    def attend_row(r, carry):
        for a, (_, dst) in enumerate(arrays):
            here = landing(dst, r, pl.ds(0, length))
            pltpu.make_async_copy(here, here, recv_sem.at[r, a]).wait()

        def widen(c, inner):
            at = pl.ds(pl.multiple_of(c * block, block), block)
            keys = k_buf[r, at, :]
            apart = jnp.where(inside(2, r, c * block, block), 0.0, FAR).astype(jnp.bfloat16)
            k_aug[0, at, :] = jnp.where(left, keys, apart)
            k_aug[1, at, :] = jnp.where(left, apart, keys)
            return inner

        lax.fori_loop(0, n_blocks, widen, 0)

        def attend_block(blk, inner):
            at = pl.ds(pl.multiple_of(blk * block, block), block)
            mine = q_buf[r, at, :]
            member = jnp.where(inside(0, r, blk * block, block), 1.0, 0.0).astype(jnp.bfloat16)
            values = v_buf[r]
            heads = []
            for h in range(2):
                ask = jnp.where(left, mine, member) if h == 0 else jnp.where(left, member, mine)
                scores = lax.dot_general(
                    ask, k_aug[h], (((1,), (1,)), ((), ())), preferred_element_type=jnp.float32
                )
                peak = jnp.max(scores, axis=1, keepdims=True)
                expos = jnp.exp(scores - peak).astype(jnp.bfloat16)
                summed = jnp.dot(expos, values, preferred_element_type=jnp.float32)
                heads.append(summed[:, :LANES] / summed[:, LANES:])
            o_buf[r, at, :] = jnp.where(left, heads[0], heads[1]).astype(jnp.bfloat16)

            @pl.when(blk > 0)
            def _():
                out_copies(r, blk - 1)

            return inner

        lax.fori_loop(0, n_blocks, attend_block, 0)
        out_copies(r, n_blocks - 1)
        return carry

    lax.fori_loop(0, rows, attend_row, 0)

    pltpu.make_async_copy(others, others, cnt_send_sem).wait()
    for r in range(rows):
        for a, (_, dst) in enumerate(arrays):
            most = landing(dst, r, pl.ds(0, length - span))
            pltpu.make_async_copy(most, most, send_sem.at[r, a]).wait()
        most = o_buf.at[r, pl.ds(0, length - span), :]
        pltpu.make_async_copy(most, most, out_send_sem.at[r]).wait()
    came = o_buf.at[:, pl.ds(0, length - span), :]
    pltpu.make_async_copy(came, came, out_sem).wait()


def local(queries, enc_keys, enc_values, dec_ids, enc_ids):
    size = lax.axis_size("seq")
    batch, span, inner = queries.shape
    rows, length = batch // 2, span * size
    anywhere = pl.BlockSpec(memory_space=pl.ANY)
    vmem = pl.BlockSpec(memory_space=pltpu.VMEM)
    return pl.pallas_call(
        functools.partial(kernel, size),
        out_shape=pltpu.VMEM(queries.shape, queries.dtype),
        in_specs=[anywhere, anywhere, anywhere, vmem, vmem],
        out_specs=vmem,
        scratch_shapes=[
            pltpu.VMEM((rows, length, LANES), jnp.bfloat16),
            pltpu.VMEM((rows, length, LANES), jnp.bfloat16),
            pltpu.VMEM((rows, length, 2 * LANES), jnp.bfloat16),
            pltpu.VMEM((rows, length, LANES), jnp.bfloat16),
            pltpu.VMEM((2, length, LANES), jnp.bfloat16),
            pltpu.VMEM((2, 1, LANES), jnp.int32),
            pltpu.VMEM((size, 1, LANES), jnp.int32),
            pltpu.VMEM((4, rows, LANES), jnp.int32),
            pltpu.SemaphoreType.DMA((rows, 3)),
            pltpu.SemaphoreType.DMA((rows, 3)),
            pltpu.SemaphoreType.DMA,
            pltpu.SemaphoreType.DMA,
            pltpu.SemaphoreType.DMA((rows,)),
            pltpu.SemaphoreType.DMA,
            pltpu.SemaphoreType.REGULAR((size // RING_X // 2 + RING_X // 2 - 1,)),
        ],
        compiler_params=pltpu.CompilerParams(
            collective_id=0, has_side_effects=True, vmem_limit_bytes=56 * 1024 * 1024
        ),
    )(queries, enc_keys, enc_values, dec_ids, enc_ids)


def solution(mesh):
    spec, id_spec = P("dp", "seq", None), P("dp", "seq")
    return jax.shard_map(
        local, mesh=mesh, in_specs=(spec, spec, spec, id_spec, id_spec), out_specs=spec, check_vma=False
    )
```

```python
import functools

import jax
import jax.numpy as jnp
from jax import lax
from jax.experimental import pallas as pl
from jax.experimental.pallas import tpu as pltpu
from jax.sharding import PartitionSpec as P

HEAD_DIM = 64
LANES = 128
NDOC = 16
RING_X = 4
FAR = -float(2**30)
MESH = pl.DeviceIdType.MESH


def doc_counts(ids, base, slot):
    counts = jnp.zeros((ids.shape[0], LANES), jnp.int32)
    for d in range(1, NDOC):
        below = jnp.sum(jnp.where(ids < d, 1, 0), axis=1, keepdims=True)
        counts = jnp.where(slot == base + d, below, counts)
    return counts


def kernel(
    size, q_ref, k_ref, v_ref, dec_ref, enc_ref, out_ref,
    q_buf, k_buf, v_buf, o_buf, k_aug, cnt, gath, edges,
    send_sem, recv_sem, cnt_send_sem, cnt_sem, out_send_sem, out_sem, round_sem,
):
    me = lax.axis_index("seq")
    rows, span = q_buf.shape[0], q_ref.shape[1]
    length = q_buf.shape[1]
    block = min(256, length)
    per_block = block // span
    n_blocks = length // block
    my_half = lax.rem(me, 2)
    ring_z, rounds = size // RING_X, round_sem.shape[0]

    def lanes_of(t):
        return pl.ds(pl.multiple_of((t // 2) * LANES, LANES), LANES)

    def span_of(t):
        return pl.ds(pl.multiple_of(t * span, span), span)

    def place(dz, dx):
        return lax.rem(me // RING_X + dz, ring_z) * RING_X + lax.rem(lax.rem(me, RING_X) + dx, RING_X)

    neighbours = (place(1, 0), place(ring_z - 1, 0), place(0, 1), place(0, RING_X - 1))

    def greet(sem):
        for t in neighbours:
            pl.semaphore_signal(sem, inc=1, device_id={"seq": t}, device_id_type=MESH)

    barrier = pltpu.get_barrier_semaphore()
    greet(barrier)

    arrays = ((k_ref, k_buf), (q_ref, q_buf), (v_ref, v_buf))

    def landing(buf, r, where):
        return buf.at[r, where, pl.ds(0, LANES)]

    for r in range(rows):
        for a, (src, dst) in enumerate(arrays):
            pltpu.make_async_copy(
                src.at[my_half * rows + r, :, lanes_of(me)],
                landing(dst, r, span_of(me)),
                recv_sem.at[r, a],
            ).start()

    lane8 = lax.broadcasted_iota(jnp.int32, (2 * rows, LANES), 1)
    row8 = lax.broadcasted_iota(jnp.int32, (2 * rows, LANES), 0)
    counts = doc_counts(dec_ref[...], 0, lane8 % (2 * NDOC)) + doc_counts(enc_ref[...], NDOC, lane8 % (2 * NDOC))
    for half in range(2):
        kept = (row8 // rows == half) & (lane8 // (2 * NDOC) == row8 % rows)
        line = jnp.sum(jnp.where(kept, counts, 0), axis=0, keepdims=True)
        cnt[half] = line

        @pl.when(my_half == half)
        def _():
            gath[me] = line
    def send_counts(t):
        pltpu.make_async_remote_copy(
            src_ref=cnt.at[lax.rem(t, 2)], dst_ref=gath.at[me],
            send_sem=cnt_send_sem, recv_sem=cnt_sem, device_id={"seq": t}, device_id_type=MESH,
        ).start()

    def send(t, r, a):
        src, dst = arrays[a]
        pltpu.make_async_remote_copy(
            src_ref=src.at[lax.rem(t, 2) * rows + r, :, lanes_of(t)],
            dst_ref=landing(dst, r, span_of(me)),
            send_sem=send_sem.at[r, a], recv_sem=recv_sem.at[r, a],
            device_id={"seq": t}, device_id_type=MESH,
        ).start()

    def each_at(nearest, farthest, act):
        def step(t, carry):
            dz = lax.rem(t // RING_X - me // RING_X + ring_z, ring_z)
            dx = lax.rem(lax.rem(t, RING_X) - lax.rem(me, RING_X) + RING_X, RING_X)
            hops = jnp.minimum(dz, ring_z - dz) + jnp.minimum(dx, RING_X - dx)

            @pl.when((hops >= nearest) & (hops <= farthest))
            def _():
                act(t)

            return carry

        lax.fori_loop(0, size, step, 0)

    def send_row(r, nearest, farthest):
        for a in range(3):
            each_at(nearest, farthest, lambda t: send(t, r, a))

    pl.semaphore_wait(barrier, 4)
    greet(round_sem.at[0])
    for r in range(rows):
        for a in range(3):
            for t in neighbours:
                send(t, r, a)
    for t in neighbours:
        send_counts(t)
    pl.semaphore_wait(round_sem.at[0], 4)
    greet(round_sem.at[1])
    each_at(2, 2, send_counts)
    send_row(0, 2, 2)
    for k in range(1, rounds):
        pl.semaphore_wait(round_sem.at[k], 4)
        if k + 1 < rounds:
            greet(round_sem.at[k + 1])
    each_at(3, size, send_counts)
    send_row(0, 3, size)
    for r in range(1, rows):
        send_row(r, 2, size)
    v_buf[:, :, LANES:] = jnp.ones((rows, length, LANES), jnp.bfloat16)

    others = gath.at[pl.ds(0, size - 1)]
    pltpu.make_async_copy(others, others, cnt_sem).wait()
    total = jnp.broadcast_to(jnp.sum(gath[...], axis=0), (8, LANES))
    slot = lax.broadcasted_iota(jnp.int32, (8, LANES), 1)
    for r in range(rows):
        for which in range(2):
            base = (2 * r + which) * NDOC
            low = pltpu.roll(total, (LANES - base) % LANES, 1)
            low = jnp.where(slot < HEAD_DIM, low, pltpu.roll(low, HEAD_DIM, 1))
            high = jnp.where(slot % HEAD_DIM == NDOC - 1, length, pltpu.roll(low, LANES - 1, 1))
            real = slot % HEAD_DIM < NDOC
            edges[2 * which, pl.ds(r, 1), :] = jnp.where(real, low, 2 * length)[:1]
            edges[2 * which + 1, pl.ds(r, 1), :] = jnp.where(real, high, 0)[:1]

    def inside(first, r, start, count):
        pos = lax.broadcasted_iota(jnp.int32, (count, LANES), 0) + start
        low = edges[first, pl.ds(r, 1), :]
        high = edges[first + 1, pl.ds(r, 1), :]
        return (pos >= low) & (pos < high)

    def out_copies(r, blk):
        for i in range(per_block):
            t = blk * per_block + i
            src = o_buf.at[r, span_of(t), :]
            dst = out_ref.at[my_half * rows + r, :, lanes_of(me)]

            @pl.when(t != me)
            def _():
                pltpu.make_async_remote_copy(
                    src_ref=src, dst_ref=dst, send_sem=out_send_sem.at[r], recv_sem=out_sem,
                    device_id={"seq": t}, device_id_type=MESH,
                ).start()

            @pl.when(t == me)
            def _():
                out_ref[my_half * rows + r, :, lanes_of(me)] = o_buf[r, span_of(me), :]

    left = lax.broadcasted_iota(jnp.int32, (block, LANES), 1) < HEAD_DIM

    def attend_row(r, carry):
        for a, (_, dst) in enumerate(arrays):
            here = landing(dst, r, pl.ds(0, length))
            pltpu.make_async_copy(here, here, recv_sem.at[r, a]).wait()

        def widen(c, inner):
            at = pl.ds(pl.multiple_of(c * block, block), block)
            keys = k_buf[r, at, :]
            apart = jnp.where(inside(2, r, c * block, block), 0.0, FAR).astype(jnp.bfloat16)
            k_aug[0, at, :] = jnp.where(left, keys, apart)
            k_aug[1, at, :] = jnp.where(left, apart, keys)
            return inner

        lax.fori_loop(0, n_blocks, widen, 0)

        def attend_block(blk, inner):
            at = pl.ds(pl.multiple_of(blk * block, block), block)
            mine = q_buf[r, at, :]
            member = jnp.where(inside(0, r, blk * block, block), 1.0, 0.0).astype(jnp.bfloat16)
            values = v_buf[r]
            heads = []
            for h in range(2):
                ask = jnp.where(left, mine, member) if h == 0 else jnp.where(left, member, mine)
                scores = lax.dot_general(
                    ask, k_aug[h], (((1,), (1,)), ((), ())), preferred_element_type=jnp.float32
                )
                peak = jnp.max(scores, axis=1, keepdims=True)
                expos = jnp.exp(scores - peak).astype(jnp.bfloat16)
                summed = jnp.dot(expos, values, preferred_element_type=jnp.float32)
                heads.append(summed[:, :LANES] / summed[:, LANES:])
            o_buf[r, at, :] = jnp.where(left, heads[0], heads[1]).astype(jnp.bfloat16)

            @pl.when(blk > 0)
            def _():
                out_copies(r, blk - 1)

            return inner

        lax.fori_loop(0, n_blocks, attend_block, 0)
        out_copies(r, n_blocks - 1)
        return carry

    lax.fori_loop(0, rows, attend_row, 0)

    pltpu.make_async_copy(others, others, cnt_send_sem).wait()
    for r in range(rows):
        for a, (_, dst) in enumerate(arrays):
            most = landing(dst, r, pl.ds(0, length - span))
            pltpu.make_async_copy(most, most, send_sem.at[r, a]).wait()
        most = o_buf.at[r, pl.ds(0, length - span), :]
        pltpu.make_async_copy(most, most, out_send_sem.at[r]).wait()
    came = o_buf.at[:, pl.ds(0, length - span), :]
    pltpu.make_async_copy(came, came, out_sem).wait()


def local(queries, enc_keys, enc_values, dec_ids, enc_ids):
    size = lax.axis_size("seq")
    batch, span, inner = queries.shape
    rows, length = batch // 2, span * size
    anywhere = pl.BlockSpec(memory_space=pl.ANY)
    vmem = pl.BlockSpec(memory_space=pltpu.VMEM)
    return pl.pallas_call(
        functools.partial(kernel, size),
        out_shape=pltpu.VMEM(queries.shape, queries.dtype),
        in_specs=[anywhere, anywhere, anywhere, vmem, vmem],
        out_specs=vmem,
        scratch_shapes=[
            pltpu.VMEM((rows, length, LANES), jnp.bfloat16),
            pltpu.VMEM((rows, length, LANES), jnp.bfloat16),
            pltpu.VMEM((rows, length, 2 * LANES), jnp.bfloat16),
            pltpu.VMEM((rows, length, LANES), jnp.bfloat16),
            pltpu.VMEM((2, length, LANES), jnp.bfloat16),
            pltpu.VMEM((2, 1, LANES), jnp.int32),
            pltpu.VMEM((size, 1, LANES), jnp.int32),
            pltpu.VMEM((4, rows, LANES), jnp.int32),
            pltpu.SemaphoreType.DMA((rows, 3)),
            pltpu.SemaphoreType.DMA((rows, 3)),
            pltpu.SemaphoreType.DMA,
            pltpu.SemaphoreType.DMA,
            pltpu.SemaphoreType.DMA((rows,)),
            pltpu.SemaphoreType.DMA,
            pltpu.SemaphoreType.REGULAR((size // RING_X // 2 + RING_X // 2 - 1,)),
        ],
        compiler_params=pltpu.CompilerParams(
            collective_id=0, has_side_effects=True, vmem_limit_bytes=56 * 1024 * 1024
        ),
    )(queries, enc_keys, enc_values, dec_ids, enc_ids)


def solution(mesh):
    spec, id_spec = P("dp", "seq", None), P("dp", "seq")
    return jax.shard_map(
        local, mesh=mesh, in_specs=(spec, spec, spec, id_spec, id_spec), out_specs=spec, check_vma=False
    )
```

```python
import functools

import jax
import jax.numpy as jnp
from jax import lax
from jax.experimental import pallas as pl
from jax.experimental.pallas import tpu as pltpu
from jax.sharding import PartitionSpec as P

HEAD_DIM = 64
LANES = 128
NDOC = 16
RING_X = 4
FAR = -float(2**30)
MESH = pl.DeviceIdType.MESH


def doc_counts(ids, base, slot):
    counts = jnp.zeros((ids.shape[0], LANES), jnp.int32)
    for d in range(1, NDOC):
        below = jnp.sum(jnp.where(ids < d, 1, 0), axis=1, keepdims=True)
        counts = jnp.where(slot == base + d, below, counts)
    return counts


def kernel(
    size, q_ref, k_ref, v_ref, dec_ref, enc_ref, out_ref,
    q_buf, k_buf, v_buf, o_buf, k_aug, cnt, gath, edges,
    send_sem, recv_sem, cnt_send_sem, cnt_sem, out_send_sem, out_sem, round_sem,
):
    me = lax.axis_index("seq")
    rows, span = q_buf.shape[0], q_ref.shape[1]
    length = q_buf.shape[1]
    block = min(256, length)
    per_block = block // span
    n_blocks = length // block
    my_half = lax.rem(me, 2)
    ring_z, rounds = size // RING_X, round_sem.shape[0]

    def lanes_of(t):
        return pl.ds(pl.multiple_of((t // 2) * LANES, LANES), LANES)

    def span_of(t):
        return pl.ds(pl.multiple_of(t * span, span), span)

    def place(dz, dx):
        return lax.rem(me // RING_X + dz, ring_z) * RING_X + lax.rem(lax.rem(me, RING_X) + dx, RING_X)

    neighbours = (place(1, 0), place(ring_z - 1, 0), place(0, 1), place(0, RING_X - 1))

    def greet(sem):
        for t in neighbours:
            pl.semaphore_signal(sem, inc=1, device_id={"seq": t}, device_id_type=MESH)

    barrier = pltpu.get_barrier_semaphore()
    greet(barrier)

    arrays = ((k_ref, k_buf), (q_ref, q_buf), (v_ref, v_buf))

    def landing(buf, r, where):
        return buf.at[r, where, pl.ds(0, LANES)]

    for r in range(rows):
        for a, (src, dst) in enumerate(arrays):
            pltpu.make_async_copy(
                src.at[my_half * rows + r, :, lanes_of(me)],
                landing(dst, r, span_of(me)),
                recv_sem.at[r, a],
            ).start()

    lane8 = lax.broadcasted_iota(jnp.int32, (2 * rows, LANES), 1)
    row8 = lax.broadcasted_iota(jnp.int32, (2 * rows, LANES), 0)
    counts = doc_counts(dec_ref[...], 0, lane8 % (2 * NDOC)) + doc_counts(enc_ref[...], NDOC, lane8 % (2 * NDOC))
    for half in range(2):
        kept = (row8 // rows == half) & (lane8 // (2 * NDOC) == row8 % rows)
        line = jnp.sum(jnp.where(kept, counts, 0), axis=0, keepdims=True)
        cnt[half] = line

        @pl.when(my_half == half)
        def _():
            gath[me] = line
    def send_counts(t):
        pltpu.make_async_remote_copy(
            src_ref=cnt.at[lax.rem(t, 2)], dst_ref=gath.at[me],
            send_sem=cnt_send_sem, recv_sem=cnt_sem, device_id={"seq": t}, device_id_type=MESH,
        ).start()

    def send(t, r, a):
        src, dst = arrays[a]
        pltpu.make_async_remote_copy(
            src_ref=src.at[lax.rem(t, 2) * rows + r, :, lanes_of(t)],
            dst_ref=landing(dst, r, span_of(me)),
            send_sem=send_sem.at[r, a], recv_sem=recv_sem.at[r, a],
            device_id={"seq": t}, device_id_type=MESH,
        ).start()

    def each_at(nearest, farthest, act):
        def step(t, carry):
            dz = lax.rem(t // RING_X - me // RING_X + ring_z, ring_z)
            dx = lax.rem(lax.rem(t, RING_X) - lax.rem(me, RING_X) + RING_X, RING_X)
            hops = jnp.minimum(dz, ring_z - dz) + jnp.minimum(dx, RING_X - dx)

            @pl.when((hops >= nearest) & (hops <= farthest))
            def _():
                act(t)

            return carry

        lax.fori_loop(0, size, step, 0)

    def send_row(r, nearest, farthest):
        for a in range(3):
            each_at(nearest, farthest, lambda t: send(t, r, a))

    pl.semaphore_wait(barrier, 4)
    greet(round_sem.at[0])
    for r in range(rows):
        for a in range(3):
            for t in neighbours:
                send(t, r, a)
    for t in neighbours:
        send_counts(t)
    pl.semaphore_wait(round_sem.at[0], 4)
    greet(round_sem.at[1])
    each_at(2, 2, send_counts)
    for r in range(rows):
        send_row(r, 2, 2)
    for k in range(1, rounds):
        pl.semaphore_wait(round_sem.at[k], 4)
        if k + 1 < rounds:
            greet(round_sem.at[k + 1])
    each_at(3, size, send_counts)
    send_row(0, 3, size)
    for r in range(1, rows):
        send_row(r, 3, size)
    v_buf[:, :, LANES:] = jnp.ones((rows, length, LANES), jnp.bfloat16)

    others = gath.at[pl.ds(0, size - 1)]
    pltpu.make_async_copy(others, others, cnt_sem).wait()
    total = jnp.broadcast_to(jnp.sum(gath[...], axis=0), (8, LANES))
    slot = lax.broadcasted_iota(jnp.int32, (8, LANES), 1)
    for r in range(rows):
        for which in range(2):
            base = (2 * r + which) * NDOC
            low = pltpu.roll(total, (LANES - base) % LANES, 1)
            low = jnp.where(slot < HEAD_DIM, low, pltpu.roll(low, HEAD_DIM, 1))
            high = jnp.where(slot % HEAD_DIM == NDOC - 1, length, pltpu.roll(low, LANES - 1, 1))
            real = slot % HEAD_DIM < NDOC
            edges[2 * which, pl.ds(r, 1), :] = jnp.where(real, low, 2 * length)[:1]
            edges[2 * which + 1, pl.ds(r, 1), :] = jnp.where(real, high, 0)[:1]

    def inside(first, r, start, count):
        pos = lax.broadcasted_iota(jnp.int32, (count, LANES), 0) + start
        low = edges[first, pl.ds(r, 1), :]
        high = edges[first + 1, pl.ds(r, 1), :]
        return (pos >= low) & (pos < high)

    def out_copies(r, blk):
        for i in range(per_block):
            t = blk * per_block + i
            src = o_buf.at[r, span_of(t), :]
            dst = out_ref.at[my_half * rows + r, :, lanes_of(me)]

            @pl.when(t != me)
            def _():
                pltpu.make_async_remote_copy(
                    src_ref=src, dst_ref=dst, send_sem=out_send_sem.at[r], recv_sem=out_sem,
                    device_id={"seq": t}, device_id_type=MESH,
                ).start()

            @pl.when(t == me)
            def _():
                out_ref[my_half * rows + r, :, lanes_of(me)] = o_buf[r, span_of(me), :]

    left = lax.broadcasted_iota(jnp.int32, (block, LANES), 1) < HEAD_DIM

    def attend_row(r, carry):
        for a, (_, dst) in enumerate(arrays):
            here = landing(dst, r, pl.ds(0, length))
            pltpu.make_async_copy(here, here, recv_sem.at[r, a]).wait()

        def widen(c, inner):
            at = pl.ds(pl.multiple_of(c * block, block), block)
            keys = k_buf[r, at, :]
            apart = jnp.where(inside(2, r, c * block, block), 0.0, FAR).astype(jnp.bfloat16)
            k_aug[0, at, :] = jnp.where(left, keys, apart)
            k_aug[1, at, :] = jnp.where(left, apart, keys)
            return inner

        lax.fori_loop(0, n_blocks, widen, 0)

        def attend_block(blk, inner):
            at = pl.ds(pl.multiple_of(blk * block, block), block)
            mine = q_buf[r, at, :]
            member = jnp.where(inside(0, r, blk * block, block), 1.0, 0.0).astype(jnp.bfloat16)
            values = v_buf[r]
            heads = []
            for h in range(2):
                ask = jnp.where(left, mine, member) if h == 0 else jnp.where(left, member, mine)
                scores = lax.dot_general(
                    ask, k_aug[h], (((1,), (1,)), ((), ())), preferred_element_type=jnp.float32
                )
                peak = jnp.max(scores, axis=1, keepdims=True)
                expos = jnp.exp(scores - peak).astype(jnp.bfloat16)
                summed = jnp.dot(expos, values, preferred_element_type=jnp.float32)
                heads.append(summed[:, :LANES] / summed[:, LANES:])
            o_buf[r, at, :] = jnp.where(left, heads[0], heads[1]).astype(jnp.bfloat16)

            @pl.when(blk > 0)
            def _():
                out_copies(r, blk - 1)

            return inner

        lax.fori_loop(0, n_blocks, attend_block, 0)
        out_copies(r, n_blocks - 1)
        return carry

    lax.fori_loop(0, rows, attend_row, 0)

    pltpu.make_async_copy(others, others, cnt_send_sem).wait()
    for r in range(rows):
        for a, (_, dst) in enumerate(arrays):
            most = landing(dst, r, pl.ds(0, length - span))
            pltpu.make_async_copy(most, most, send_sem.at[r, a]).wait()
        most = o_buf.at[r, pl.ds(0, length - span), :]
        pltpu.make_async_copy(most, most, out_send_sem.at[r]).wait()
    came = o_buf.at[:, pl.ds(0, length - span), :]
    pltpu.make_async_copy(came, came, out_sem).wait()


def local(queries, enc_keys, enc_values, dec_ids, enc_ids):
    size = lax.axis_size("seq")
    batch, span, inner = queries.shape
    rows, length = batch // 2, span * size
    anywhere = pl.BlockSpec(memory_space=pl.ANY)
    vmem = pl.BlockSpec(memory_space=pltpu.VMEM)
    return pl.pallas_call(
        functools.partial(kernel, size),
        out_shape=pltpu.VMEM(queries.shape, queries.dtype),
        in_specs=[anywhere, anywhere, anywhere, vmem, vmem],
        out_specs=vmem,
        scratch_shapes=[
            pltpu.VMEM((rows, length, LANES), jnp.bfloat16),
            pltpu.VMEM((rows, length, LANES), jnp.bfloat16),
            pltpu.VMEM((rows, length, 2 * LANES), jnp.bfloat16),
            pltpu.VMEM((rows, length, LANES), jnp.bfloat16),
            pltpu.VMEM((2, length, LANES), jnp.bfloat16),
            pltpu.VMEM((2, 1, LANES), jnp.int32),
            pltpu.VMEM((size, 1, LANES), jnp.int32),
            pltpu.VMEM((4, rows, LANES), jnp.int32),
            pltpu.SemaphoreType.DMA((rows, 3)),
            pltpu.SemaphoreType.DMA((rows, 3)),
            pltpu.SemaphoreType.DMA,
            pltpu.SemaphoreType.DMA,
            pltpu.SemaphoreType.DMA((rows,)),
            pltpu.SemaphoreType.DMA,
            pltpu.SemaphoreType.REGULAR((size // RING_X // 2 + RING_X // 2 - 1,)),
        ],
        compiler_params=pltpu.CompilerParams(
            collective_id=0, has_side_effects=True, vmem_limit_bytes=56 * 1024 * 1024
        ),
    )(queries, enc_keys, enc_values, dec_ids, enc_ids)


def solution(mesh):
    spec, id_spec = P("dp", "seq", None), P("dp", "seq")
    return jax.shard_map(
        local, mesh=mesh, in_specs=(spec, spec, spec, id_spec, id_spec), out_specs=spec, check_vma=False
    )
```

```python
import functools

import jax
import jax.numpy as jnp
from jax import lax
from jax.experimental import pallas as pl
from jax.experimental.pallas import tpu as pltpu
from jax.sharding import PartitionSpec as P

HEAD_DIM = 64
LANES = 128
NDOC = 16
RING_X = 4
FAR = -float(2**30)
MESH = pl.DeviceIdType.MESH


def doc_counts(ids, base, slot):
    counts = jnp.zeros((ids.shape[0], LANES), jnp.int32)
    for d in range(1, NDOC):
        below = jnp.sum(jnp.where(ids < d, 1, 0), axis=1, keepdims=True)
        counts = jnp.where(slot == base + d, below, counts)
    return counts


def kernel(
    size, q_ref, k_ref, v_ref, dec_ref, enc_ref, out_ref,
    q_buf, k_buf, v_buf, o_buf, k_aug, cnt, gath, edges,
    send_sem, recv_sem, cnt_send_sem, cnt_sem, out_send_sem, out_sem, round_sem,
):
    me = lax.axis_index("seq")
    rows, span = q_buf.shape[0], q_ref.shape[1]
    length = q_buf.shape[1]
    block = min(256, length)
    per_block = block // span
    n_blocks = length // block
    my_half = lax.rem(me, 2)
    ring_z, rounds = size // RING_X, round_sem.shape[0]

    def lanes_of(t):
        return pl.ds(pl.multiple_of((t // 2) * LANES, LANES), LANES)

    def span_of(t):
        return pl.ds(pl.multiple_of(t * span, span), span)

    def place(dz, dx):
        return lax.rem(me // RING_X + dz, ring_z) * RING_X + lax.rem(lax.rem(me, RING_X) + dx, RING_X)

    neighbours = (place(1, 0), place(ring_z - 1, 0), place(0, 1), place(0, RING_X - 1))

    def greet(sem):
        for t in neighbours:
            pl.semaphore_signal(sem, inc=1, device_id={"seq": t}, device_id_type=MESH)

    barrier = pltpu.get_barrier_semaphore()
    greet(barrier)

    arrays = ((k_ref, k_buf), (q_ref, q_buf), (v_ref, v_buf))

    def landing(buf, r, where):
        return buf.at[r, where, pl.ds(0, LANES)]

    for r in range(rows):
        for a, (src, dst) in enumerate(arrays):
            pltpu.make_async_copy(
                src.at[my_half * rows + r, :, lanes_of(me)],
                landing(dst, r, span_of(me)),
                recv_sem.at[r, a],
            ).start()

    lane8 = lax.broadcasted_iota(jnp.int32, (2 * rows, LANES), 1)
    row8 = lax.broadcasted_iota(jnp.int32, (2 * rows, LANES), 0)
    counts = doc_counts(dec_ref[...], 0, lane8 % (2 * NDOC)) + doc_counts(enc_ref[...], NDOC, lane8 % (2 * NDOC))
    for half in range(2):
        kept = (row8 // rows == half) & (lane8 // (2 * NDOC) == row8 % rows)
        line = jnp.sum(jnp.where(kept, counts, 0), axis=0, keepdims=True)
        cnt[half] = line

        @pl.when(my_half == half)
        def _():
            gath[me] = line
    def send_counts(t):
        pltpu.make_async_remote_copy(
            src_ref=cnt.at[lax.rem(t, 2)], dst_ref=gath.at[me],
            send_sem=cnt_send_sem, recv_sem=cnt_sem, device_id={"seq": t}, device_id_type=MESH,
        ).start()

    def send(t, r, a):
        src, dst = arrays[a]
        pltpu.make_async_remote_copy(
            src_ref=src.at[lax.rem(t, 2) * rows + r, :, lanes_of(t)],
            dst_ref=landing(dst, r, span_of(me)),
            send_sem=send_sem.at[r, a], recv_sem=recv_sem.at[r, a],
            device_id={"seq": t}, device_id_type=MESH,
        ).start()

    def each_at(nearest, farthest, act):
        def step(t, carry):
            dz = lax.rem(t // RING_X - me // RING_X + ring_z, ring_z)
            dx = lax.rem(lax.rem(t, RING_X) - lax.rem(me, RING_X) + RING_X, RING_X)
            hops = jnp.minimum(dz, ring_z - dz) + jnp.minimum(dx, RING_X - dx)

            @pl.when((hops >= nearest) & (hops <= farthest))
            def _():
                act(t)

            return carry

        lax.fori_loop(0, size, step, 0)

    def send_row(r, nearest, farthest):
        for a in range(3):
            each_at(nearest, farthest, lambda t: send(t, r, a))

    pl.semaphore_wait(barrier, 4)
    greet(round_sem.at[0])
    for r in range(rows):
        for a in range(3):
            for t in neighbours:
                send(t, r, a)
    for t in neighbours:
        send_counts(t)
    pl.semaphore_wait(round_sem.at[0], 4)
    greet(round_sem.at[1])
    each_at(2, 2, send_counts)
    each_at(2, 2, lambda t: [send(t, r, a) for r in range(rows) for a in range(3)])
    for k in range(1, rounds):
        pl.semaphore_wait(round_sem.at[k], 4)
        if k + 1 < rounds:
            greet(round_sem.at[k + 1])
    each_at(3, size, send_counts)
    send_row(0, 3, size)
    for r in range(1, rows):
        send_row(r, 3, size)
    v_buf[:, :, LANES:] = jnp.ones((rows, length, LANES), jnp.bfloat16)

    others = gath.at[pl.ds(0, size - 1)]
    pltpu.make_async_copy(others, others, cnt_sem).wait()
    total = jnp.broadcast_to(jnp.sum(gath[...], axis=0), (8, LANES))
    slot = lax.broadcasted_iota(jnp.int32, (8, LANES), 1)
    for r in range(rows):
        for which in range(2):
            base = (2 * r + which) * NDOC
            low = pltpu.roll(total, (LANES - base) % LANES, 1)
            low = jnp.where(slot < HEAD_DIM, low, pltpu.roll(low, HEAD_DIM, 1))
            high = jnp.where(slot % HEAD_DIM == NDOC - 1, length, pltpu.roll(low, LANES - 1, 1))
            real = slot % HEAD_DIM < NDOC
            edges[2 * which, pl.ds(r, 1), :] = jnp.where(real, low, 2 * length)[:1]
            edges[2 * which + 1, pl.ds(r, 1), :] = jnp.where(real, high, 0)[:1]

    def inside(first, r, start, count):
        pos = lax.broadcasted_iota(jnp.int32, (count, LANES), 0) + start
        low = edges[first, pl.ds(r, 1), :]
        high = edges[first + 1, pl.ds(r, 1), :]
        return (pos >= low) & (pos < high)

    def out_copies(r, blk):
        for i in range(per_block):
            t = blk * per_block + i
            src = o_buf.at[r, span_of(t), :]
            dst = out_ref.at[my_half * rows + r, :, lanes_of(me)]

            @pl.when(t != me)
            def _():
                pltpu.make_async_remote_copy(
                    src_ref=src, dst_ref=dst, send_sem=out_send_sem.at[r], recv_sem=out_sem,
                    device_id={"seq": t}, device_id_type=MESH,
                ).start()

            @pl.when(t == me)
            def _():
                out_ref[my_half * rows + r, :, lanes_of(me)] = o_buf[r, span_of(me), :]

    left = lax.broadcasted_iota(jnp.int32, (block, LANES), 1) < HEAD_DIM

    def attend_row(r, carry):
        for a, (_, dst) in enumerate(arrays):
            here = landing(dst, r, pl.ds(0, length))
            pltpu.make_async_copy(here, here, recv_sem.at[r, a]).wait()

        def widen(c, inner):
            at = pl.ds(pl.multiple_of(c * block, block), block)
            keys = k_buf[r, at, :]
            apart = jnp.where(inside(2, r, c * block, block), 0.0, FAR).astype(jnp.bfloat16)
            k_aug[0, at, :] = jnp.where(left, keys, apart)
            k_aug[1, at, :] = jnp.where(left, apart, keys)
            return inner

        lax.fori_loop(0, n_blocks, widen, 0)

        def attend_block(blk, inner):
            at = pl.ds(pl.multiple_of(blk * block, block), block)
            mine = q_buf[r, at, :]
            member = jnp.where(inside(0, r, blk * block, block), 1.0, 0.0).astype(jnp.bfloat16)
            values = v_buf[r]
            heads = []
            for h in range(2):
                ask = jnp.where(left, mine, member) if h == 0 else jnp.where(left, member, mine)
                scores = lax.dot_general(
                    ask, k_aug[h], (((1,), (1,)), ((), ())), preferred_element_type=jnp.float32
                )
                peak = jnp.max(scores, axis=1, keepdims=True)
                expos = jnp.exp(scores - peak).astype(jnp.bfloat16)
                summed = jnp.dot(expos, values, preferred_element_type=jnp.float32)
                heads.append(summed[:, :LANES] / summed[:, LANES:])
            o_buf[r, at, :] = jnp.where(left, heads[0], heads[1]).astype(jnp.bfloat16)

            @pl.when(blk > 0)
            def _():
                out_copies(r, blk - 1)

            return inner

        lax.fori_loop(0, n_blocks, attend_block, 0)
        out_copies(r, n_blocks - 1)
        return carry

    lax.fori_loop(0, rows, attend_row, 0)

    pltpu.make_async_copy(others, others, cnt_send_sem).wait()
    for r in range(rows):
        for a, (_, dst) in enumerate(arrays):
            most = landing(dst, r, pl.ds(0, length - span))
            pltpu.make_async_copy(most, most, send_sem.at[r, a]).wait()
        most = o_buf.at[r, pl.ds(0, length - span), :]
        pltpu.make_async_copy(most, most, out_send_sem.at[r]).wait()
    came = o_buf.at[:, pl.ds(0, length - span), :]
    pltpu.make_async_copy(came, came, out_sem).wait()


def local(queries, enc_keys, enc_values, dec_ids, enc_ids):
    size = lax.axis_size("seq")
    batch, span, inner = queries.shape
    rows, length = batch // 2, span * size
    anywhere = pl.BlockSpec(memory_space=pl.ANY)
    vmem = pl.BlockSpec(memory_space=pltpu.VMEM)
    return pl.pallas_call(
        functools.partial(kernel, size),
        out_shape=pltpu.VMEM(queries.shape, queries.dtype),
        in_specs=[anywhere, anywhere, anywhere, vmem, vmem],
        out_specs=vmem,
        scratch_shapes=[
            pltpu.VMEM((rows, length, LANES), jnp.bfloat16),
            pltpu.VMEM((rows, length, LANES), jnp.bfloat16),
            pltpu.VMEM((rows, length, 2 * LANES), jnp.bfloat16),
            pltpu.VMEM((rows, length, LANES), jnp.bfloat16),
            pltpu.VMEM((2, length, LANES), jnp.bfloat16),
            pltpu.VMEM((2, 1, LANES), jnp.int32),
            pltpu.VMEM((size, 1, LANES), jnp.int32),
            pltpu.VMEM((4, rows, LANES), jnp.int32),
            pltpu.SemaphoreType.DMA((rows, 3)),
            pltpu.SemaphoreType.DMA((rows, 3)),
            pltpu.SemaphoreType.DMA,
            pltpu.SemaphoreType.DMA,
            pltpu.SemaphoreType.DMA((rows,)),
            pltpu.SemaphoreType.DMA,
            pltpu.SemaphoreType.REGULAR((size // RING_X // 2 + RING_X // 2 - 1,)),
        ],
        compiler_params=pltpu.CompilerParams(
            collective_id=0, has_side_effects=True, vmem_limit_bytes=56 * 1024 * 1024
        ),
    )(queries, enc_keys, enc_values, dec_ids, enc_ids)


def solution(mesh):
    spec, id_spec = P("dp", "seq", None), P("dp", "seq")
    return jax.shard_map(
        local, mesh=mesh, in_specs=(spec, spec, spec, id_spec, id_spec), out_specs=spec, check_vma=False
    )
```
